8 devices in a mesh: data: 2 (over z, y), tp: 4 (over x, core).
Axes of the slice: x: 2, y: 2, z: 1, core: 2. Of those that a mesh axis runs over, the one named last changes fastest.
Arguments:
- x_in: bfloat16 [8192, 5120], P('data'), parts along dimension 0
- w_gate: bfloat16 [5120, 13824], P(None, 'tp')
- w_up: bfloat16 [5120, 13824], P(None, 'tp')
- w_down: bfloat16 [13824, 5120], P('tp')
- residual: bfloat16 [8192, 5120], P(('data', 'tp')), parts along dimension 0
- norm_gain: float32 [5120], replicated
Outputs:
- output 1: bfloat16 [8192, 5120], P(('data', 'tp')), parts along dimension 0
- output 2: bfloat16 [8192, 5120], P(('data', 'tp')), parts along dimension 0
There are 2 independent parts. The reference program is written for one: setup_inputs(seed, part) draws one part's arguments, and reference() takes and returns one part's arrays. A program takes and returns all parts, laid end to end along the dimension named above; an argument that names none is the same for every part.
All inputs are finite; a program needn't handle non-finite values.
Results may differ from the reference program's by a relative error of at most 0.00659832.
Values are sent between devices in bfloat16 or wider.
A program may use at most 1 GiB of HBM per device.

```python
import jax
import jax.numpy as jnp
from jax import lax

T = 4096
D = 5120
F = 13824
TP = 4
F_SHARD = F // TP
EPS = 1e-5


def setup_inputs(seed: int = 0, part: int = 0) -> dict:
    key = jax.random.key(seed)
    shared = jax.random.split(key, 4)
    local = jax.random.split(jax.random.fold_in(key, part), 2)
    x_in = jax.random.normal(local[0], (T, D), jnp.float32).astype(jnp.bfloat16)
    residual = jax.random.normal(local[1], (T, D), jnp.float32).astype(jnp.bfloat16)
    w_gate = (jax.random.normal(shared[0], (D, F), jnp.float32) * D ** -0.5).astype(jnp.bfloat16)
    w_up = (jax.random.normal(shared[1], (D, F), jnp.float32) * D ** -0.5).astype(jnp.bfloat16)
    w_down = (jax.random.normal(shared[2], (F, D), jnp.float32) * (2.0 / F) ** 0.5).astype(jnp.bfloat16)
    norm_gain = 1.0 + 0.3 * jax.random.normal(shared[3], (D,), jnp.float32)
    return {"x_in": x_in, "w_gate": w_gate, "w_up": w_up, "w_down": w_down, "residual": residual, "norm_gain": norm_gain}


def reference(x_in, w_gate, w_up, w_down, residual, norm_gain):
    gate_shards = w_gate.reshape(D, TP, F_SHARD).transpose(1, 0, 2)
    up_shards = w_up.reshape(D, TP, F_SHARD).transpose(1, 0, 2)
    down_shards = w_down.reshape(TP, F_SHARD, D)

    def add_shard(running, shard_w):
        gate_cols, up_cols, down_rows = shard_w
        gate_val = jnp.dot(x_in, gate_cols, preferred_element_type=jnp.float32)
        up_val = jnp.dot(x_in, up_cols, preferred_element_type=jnp.float32)
        hidden = (jax.nn.silu(gate_val) * up_val).astype(jnp.bfloat16)
        part_prod = jnp.dot(hidden, down_rows, preferred_element_type=jnp.float32).astype(jnp.bfloat16)
        return running + part_prod.astype(jnp.float32), None

    y_sum = lax.scan(add_shard, jnp.zeros((T, D), jnp.float32), (gate_shards, up_shards, down_shards))[0]
    hidden_sum = residual.astype(jnp.float32) + y_sum
    mean_sq = jnp.mean(hidden_sum * hidden_sum, axis=-1, keepdims=True)
    normed = hidden_sum * lax.rsqrt(mean_sq + EPS) * norm_gain
    return hidden_sum.astype(jnp.bfloat16), normed.astype(jnp.bfloat16)
```

```python
import functools

import jax
import jax.numpy as jnp
from jax import lax
from jax.experimental import pallas as pl
from jax.experimental.pallas import tpu as pltpu
from jax.sharding import PartitionSpec as P

EPS = 1e-5
TF = 384
TD = 512
CHUNKS = (128, 256, 512, 128)
VMEM = 67043328


def gate_up(x, w_gate, w_up, hidden, step):
    width = w_gate.shape[1]
    x_val = x[...]
    for piece in range(width // 128):
        cols = slice(piece * 128, piece * 128 + 128)
        both = jnp.concatenate([w_gate[:, cols], w_up[:, cols]], axis=1)
        prod = jnp.dot(x_val, both, preferred_element_type=jnp.float32)
        val = (jax.nn.silu(prod[:, :128]) * prod[:, 128:]).astype(jnp.bfloat16)
        start = pl.multiple_of(step * width + piece * 128, 128)
        hidden[:, pl.ds(start, 128)] = val


def cost(rows, d_model, d_hidden):
    return pl.CostEstimate(flops=6 * rows * d_model * d_hidden, bytes_accessed=6 * d_model * d_hidden, transcendentals=rows * d_hidden)


def partial_kernel(nf, sizes, starts, x_hbm, w_gate, w_up, w_down, after, y_a, y_b, x, hidden, sem):
    del after
    step = pl.program_id(0)

    @pl.when(step == 0)
    def _():
        copies = []
        for k in range(2):
            row = pl.multiple_of(starts[k], 128)
            copies.append(pltpu.make_async_copy(x_hbm.at[pl.ds(row, sizes[k])], x.at[pl.ds(k * sizes[0], sizes[k])], sem.at[k]))
        for copy in copies:
            copy.start()
        for copy in copies:
            copy.wait()

    @pl.when(step < nf)
    def _():
        gate_up(x, w_gate, w_up, hidden, step)

    @pl.when(step >= nf)
    def _():
        prod = jnp.dot(hidden[...], w_down[...], preferred_element_type=jnp.float32).astype(jnp.bfloat16)
        y_a[...] = prod[: sizes[0]]
        y_b[...] = prod[sizes[0] :]


def partial_rows(sizes, starts, x_in, w_gate, w_up, w_down, after):
    d_model, d_hidden = w_gate.shape
    nf, nd = d_hidden // TF, d_model // TD
    rows = sum(sizes)
    return pl.pallas_call(
        functools.partial(partial_kernel, nf, sizes),
        grid_spec=pltpu.PrefetchScalarGridSpec(
            num_scalar_prefetch=1,
            grid=(nf + nd,),
            in_specs=[
                pl.BlockSpec(memory_space=pl.ANY),
                pl.BlockSpec((d_model, TF), lambda s, _: (0, jnp.minimum(s, nf - 1))),
                pl.BlockSpec((d_model, TF), lambda s, _: (0, jnp.minimum(s, nf - 1))),
                pl.BlockSpec((d_hidden, TD), lambda s, _: (0, jnp.maximum(s - nf, 0))),
                pl.BlockSpec(memory_space=pl.ANY),
            ],
            out_specs=[pl.BlockSpec((size, TD), lambda s, _: (0, jnp.maximum(s - nf, 0))) for size in sizes],
            scratch_shapes=[
                pltpu.VMEM((rows, d_model), jnp.bfloat16),
                pltpu.VMEM((rows, d_hidden), jnp.bfloat16),
                pltpu.SemaphoreType.DMA((2,)),
            ],
        ),
        out_shape=[jax.ShapeDtypeStruct((size, d_model), jnp.bfloat16) for size in sizes],
        compiler_params=pltpu.CompilerParams(vmem_limit_bytes=VMEM),
        cost_estimate=cost(rows, d_model, d_hidden),
        name=f"partial_{rows}",
    )(starts, x_in, w_gate, w_up, w_down, after)


def own_kernel(nf, nd, rows, first, sizes, starts, x_hbm, w_gate, w_up, w_down, gain, residual, *rest):
    n_in = 1 + 2 * len(sizes)
    received, rest = rest[:n_in], rest[n_in:]
    if first:
        (h_out, n_out), rest = rest[:2], rest[2:]
    else:
        (_, n_alias, h_out, n_out), rest = rest[:4], rest[4:]
    x, hidden, total, square, n_buf, sem, out_sem = rest
    step = pl.program_id(0)
    width = w_down.shape[1]

    @pl.when(step == 0)
    def _():
        row = pl.multiple_of(starts[0], 128)
        copy = pltpu.make_async_copy(x_hbm.at[pl.ds(row, rows)], x, sem)
        copy.start()
        copy.wait()
        square[...] = jnp.zeros_like(square)

    @pl.when(step < nf)
    def _():
        gate_up(x, w_gate, w_up, hidden, step)

    @pl.when(step >= nf)
    def _():
        prod = jnp.dot(hidden[...], w_down[...], preferred_element_type=jnp.float32)
        prod = prod.astype(jnp.bfloat16).astype(jnp.float32)
        at = 0
        cols = pl.ds(pl.multiple_of((step - nf) * width, width), width)
        for k, size in enumerate(sizes):
            part = prod[at : at + size]
            here = pl.ds(at, size)
            part = part + received[0][here, :].astype(jnp.float32)
            for r in received[2 * k + 1 : 2 * k + 3]:
                part = part + r[...].astype(jnp.float32)
            part = residual[here, :].astype(jnp.float32) + part
            total[here, cols] = part
            h_out[here, :] = part.astype(jnp.bfloat16)
            sq = part * part
            acc = square[here, :]
            for c in range(width // 128):
                acc = acc + sq[:, c * 128 : c * 128 + 128]
            square[here, :] = acc
            at += size

    @pl.when(step == nf + nd - 1)
    def _():
        d_model = gain.shape[1]
        mean_sq = jnp.sum(square[...], axis=1, keepdims=True) / d_model
        scale = lax.rsqrt(mean_sq + EPS)
        out_row = 0 if first else 1024 - rows

        copies = []
        n_parts = rows // 128
        for c in range(n_parts):
            here = pl.ds(c * 128, 128)
            n_buf[here, :] = (total[here, :] * scale[c * 128 : c * 128 + 128] * gain[...]).astype(jnp.bfloat16)
            copy = pltpu.make_async_copy(n_buf.at[here], n_out.at[pl.ds(out_row + c * 128, 128)], out_sem.at[c])
            copy.start()
            copies.append(copy)
        for copy in copies:
            copy.wait()


def own_rows(rows, row0, sizes, starts, x_in, w_gate, w_up, w_down, gain, residual, received, previous):
    d_model, d_hidden = w_gate.shape
    td = 256
    nf, nd = d_hidden // TF, d_model // td
    col = lambda s, _: (0, jnp.maximum(s - nf, 0))
    tile = lambda s, _: (row0, jnp.maximum(s - nf, 0) * td)
    out = jax.ShapeDtypeStruct((1024, d_model), jnp.bfloat16)
    any_spec = pl.BlockSpec(memory_space=pl.ANY)
    n_prev = 0 if previous is None else 2
    n_fixed = 7
    return pl.pallas_call(
        functools.partial(own_kernel, nf, nd, rows, previous is None, sizes),
        grid_spec=pltpu.PrefetchScalarGridSpec(
            num_scalar_prefetch=1,
            grid=(nf + nd,),
            in_specs=[
                any_spec,
                pl.BlockSpec((d_model, TF), lambda s, _: (0, jnp.minimum(s, nf - 1))),
                pl.BlockSpec((d_model, TF), lambda s, _: (0, jnp.minimum(s, nf - 1))),
                pl.BlockSpec((d_hidden, td), col),
                pl.BlockSpec((1, d_model), lambda s, _: (0, 0)),
                pl.BlockSpec((pl.Element(rows), pl.Element(td)), tile),
            ]
            + [pl.BlockSpec((size, td), col) for size in (rows,) + tuple(s for s in sizes for _ in range(2))]
            + [any_spec] * n_prev,
            out_specs=[pl.BlockSpec((pl.Element(rows), pl.Element(td)), tile), any_spec],
            scratch_shapes=[
                pltpu.VMEM((rows, d_model), jnp.bfloat16),
                pltpu.VMEM((rows, d_hidden), jnp.bfloat16),
                pltpu.VMEM((rows, d_model), jnp.float32),
                pltpu.VMEM((rows, 128), jnp.float32),
                pltpu.VMEM((rows, d_model), jnp.bfloat16),
                pltpu.SemaphoreType.DMA,
                pltpu.SemaphoreType.DMA((rows // 128,)),
            ],
        ),
        out_shape=[out, out],
        input_output_aliases={} if previous is None else {n_fixed + 1 + 2 * len(sizes): 0, n_fixed + 1 + 2 * len(sizes) + 1: 1},
        compiler_params=pltpu.CompilerParams(vmem_limit_bytes=VMEM),
        cost_estimate=cost(rows, d_model, d_hidden),
        name=f"own_{row0}",
    )(starts, x_in, w_gate, w_up, w_down, gain, residual, *received, *(previous or ()))


def solution(mesh):
    straight = [(p, (p + 2) % 4) for p in range(4)]
    crossed = [(p, (p + 2) % 4 ^ 1) for p in range(4)]
    partner_of = [(p, p ^ 1) for p in range(4)]

    def local_block(x_in, w_gate, w_up, w_down, residual, norm_gain):
        me = lax.axis_index("tp")
        weights = (x_in, w_gate, w_up, w_down)
        dest_a = ((me + 2) % 4) * 1024
        dest_b = ((me + 2) % 4 ^ 1) * 1024
        partner = (me ^ 1) * 1024
        recv = []
        at = 0
        y_a = x_in
        for half in CHUNKS:
            y_a, y_b = partial_rows((half, half), jnp.stack([dest_a + at, dest_b + at]), *weights, y_a)
            recv.append((lax.ppermute(y_a, "tp", straight), lax.ppermute(y_b, "tp", crossed)))
            at += half
        cut = CHUNKS[0] + CHUNKS[1]
        near = partial_rows((cut, 1024 - cut), jnp.stack([partner, partner + cut]), *weights, y_a)
        near = [lax.ppermute(y, "tp", partner_of) for y in near]
        gain = norm_gain.reshape(1, -1)
        outs = None
        for k, (row0, rows) in enumerate(((0, cut), (cut, 1024 - cut))):
            pieces = [near[k], *recv[2 * k], *recv[2 * k + 1]]
            start = jnp.stack([me * 1024 + row0])
            outs = own_rows(rows, row0, CHUNKS[2 * k : 2 * k + 2], start, *weights, gain, residual, pieces, outs)
        return tuple(outs)

    row_spec = P(("data", "tp"), None)
    return jax.shard_map(local_block, mesh=mesh, in_specs=(P("data", None), P(None, "tp"), P(None, "tp"), P("tp", None), row_spec, P(None)), out_specs=(row_spec, row_spec), check_vma=False)
```

```python
import functools

import jax
import jax.numpy as jnp
from jax import lax
from jax.experimental import pallas as pl
from jax.experimental.pallas import tpu as pltpu
from jax.sharding import PartitionSpec as P


EPS = 1e-5
TF = 384
TD = 512
CHUNKS = (128, 256, 512, 128)
VMEM = 67043328


def gate_up(x, w_gate, w_up, hidden, step):
    width = w_gate.shape[1]
    x_val = x[...]
    for piece in range(width // 128):
        cols = slice(piece * 128, piece * 128 + 128)
        both = jnp.concatenate([w_gate[:, cols], w_up[:, cols]], axis=1)
        prod = jnp.dot(x_val, both, preferred_element_type=jnp.float32)
        val = (jax.nn.silu(prod[:, :128]) * prod[:, 128:]).astype(jnp.bfloat16)
        start = pl.multiple_of(step * width + piece * 128, 128)
        hidden[:, pl.ds(start, 128)] = val


def cost(rows, d_model, d_hidden):
    return pl.CostEstimate(flops=6 * rows * d_model * d_hidden, bytes_accessed=6 * d_model * d_hidden, transcendentals=rows * d_hidden)


def partial_kernel(nf, sizes, starts, x_hbm, w_gate, w_up, w_down, after, y_a, y_b, x, hidden, sem):
    del after
    step = pl.program_id(0)

    @pl.when(step == 0)
    def _():
        copies = []
        for k in range(2):
            row = pl.multiple_of(starts[k], 128)
            copies.append(pltpu.make_async_copy(x_hbm.at[pl.ds(row, sizes[k])], x.at[pl.ds(k * sizes[0], sizes[k])], sem.at[k]))
        for copy in copies:
            copy.start()
        for copy in copies:
            copy.wait()

    @pl.when(step < nf)
    def _():
        gate_up(x, w_gate, w_up, hidden, step)

    @pl.when(step >= nf)
    def _():
        prod = jnp.dot(hidden[...], w_down[...], preferred_element_type=jnp.float32).astype(jnp.bfloat16)
        y_a[...] = prod[: sizes[0]]
        y_b[...] = prod[sizes[0] :]


def partial_rows(sizes, starts, x_in, w_gate, w_up, w_down, after):
    d_model, d_hidden = w_gate.shape
    nf, nd = d_hidden // TF, d_model // TD
    rows = sum(sizes)
    return pl.pallas_call(
        functools.partial(partial_kernel, nf, sizes),
        grid_spec=pltpu.PrefetchScalarGridSpec(
            num_scalar_prefetch=1,
            grid=(nf + nd,),
            in_specs=[
                pl.BlockSpec(memory_space=pl.ANY),
                pl.BlockSpec((d_model, TF), lambda s, _: (0, jnp.minimum(s, nf - 1))),
                pl.BlockSpec((d_model, TF), lambda s, _: (0, jnp.minimum(s, nf - 1))),
                pl.BlockSpec((d_hidden, TD), lambda s, _: (0, jnp.maximum(s - nf, 0))),
                pl.BlockSpec(memory_space=pl.ANY),
            ],
            out_specs=[pl.BlockSpec((size, TD), lambda s, _: (0, jnp.maximum(s - nf, 0))) for size in sizes],
            scratch_shapes=[
                pltpu.VMEM((rows, d_model), jnp.bfloat16),
                pltpu.VMEM((rows, d_hidden), jnp.bfloat16),
                pltpu.SemaphoreType.DMA((2,)),
            ],
        ),
        out_shape=[jax.ShapeDtypeStruct((size, d_model), jnp.bfloat16) for size in sizes],
        compiler_params=pltpu.CompilerParams(vmem_limit_bytes=VMEM),
        cost_estimate=cost(rows, d_model, d_hidden),
    )(starts, x_in, w_gate, w_up, w_down, after)


def own_kernel(nf, nd, rows, first, sizes, starts, x_hbm, w_gate, w_up, w_down, gain, residual, *rest):
    n_in = 1 + 2 * len(sizes)
    received, rest = rest[:n_in], rest[n_in:]
    if first:
        (h_out, n_out), rest = rest[:2], rest[2:]
    else:
        (_, n_alias, h_out, n_out), rest = rest[:4], rest[4:]
    x, hidden, total, square, n_buf, sem, out_sem = rest
    step = pl.program_id(0)
    width = w_down.shape[1]

    @pl.when(step == 0)
    def _():
        row = pl.multiple_of(starts[0], 128)
        copy = pltpu.make_async_copy(x_hbm.at[pl.ds(row, rows)], x, sem)
        copy.start()
        copy.wait()
        square[...] = jnp.zeros_like(square)

    @pl.when(step < nf)
    def _():
        gate_up(x, w_gate, w_up, hidden, step)

    @pl.when(step >= nf)
    def _():
        prod = jnp.dot(hidden[...], w_down[...], preferred_element_type=jnp.float32)
        prod = prod.astype(jnp.bfloat16).astype(jnp.float32)
        at = 0
        cols = pl.ds(pl.multiple_of((step - nf) * width, width), width)
        for k, size in enumerate(sizes):
            part = prod[at : at + size]
            here = pl.ds(at, size)
            part = part + received[0][here, :].astype(jnp.float32)
            for r in received[2 * k + 1 : 2 * k + 3]:
                part = part + r[...].astype(jnp.float32)
            part = residual[here, :].astype(jnp.float32) + part
            total[here, cols] = part
            h_out[here, :] = part.astype(jnp.bfloat16)
            sq = part * part
            acc = square[here, :]
            for c in range(width // 128):
                acc = acc + sq[:, c * 128 : c * 128 + 128]
            square[here, :] = acc
            at += size

    @pl.when(step == nf + nd - 1)
    def _():
        d_model = gain.shape[1]
        mean_sq = jnp.sum(square[...], axis=1, keepdims=True) / d_model
        scale = lax.rsqrt(mean_sq + EPS)
        out_row = 0 if first else 1024 - rows

        copies = []
        n_parts = rows // 128
        for c in range(n_parts):
            here = pl.ds(c * 128, 128)
            n_buf[here, :] = (total[here, :] * scale[c * 128 : c * 128 + 128] * gain[...]).astype(jnp.bfloat16)
            copy = pltpu.make_async_copy(n_buf.at[here], n_out.at[pl.ds(out_row + c * 128, 128)], out_sem.at[c])
            copy.start()
            copies.append(copy)
        for copy in copies:
            copy.wait()


def own_rows(rows, row0, sizes, starts, x_in, w_gate, w_up, w_down, gain, residual, received, previous):
    d_model, d_hidden = w_gate.shape
    td = 256
    nf, nd = d_hidden // TF, d_model // td
    col = lambda s, _: (0, jnp.maximum(s - nf, 0))
    tile = lambda s, _: (row0, jnp.maximum(s - nf, 0) * td)
    out = jax.ShapeDtypeStruct((1024, d_model), jnp.bfloat16)
    any_spec = pl.BlockSpec(memory_space=pl.ANY)
    n_prev = 0 if previous is None else 2
    n_fixed = 7
    return pl.pallas_call(
        functools.partial(own_kernel, nf, nd, rows, previous is None, sizes),
        grid_spec=pltpu.PrefetchScalarGridSpec(
            num_scalar_prefetch=1,
            grid=(nf + nd,),
            in_specs=[
                any_spec,
                pl.BlockSpec((d_model, TF), lambda s, _: (0, jnp.minimum(s, nf - 1))),
                pl.BlockSpec((d_model, TF), lambda s, _: (0, jnp.minimum(s, nf - 1))),
                pl.BlockSpec((d_hidden, td), col),
                pl.BlockSpec((1, d_model), lambda s, _: (0, 0)),
                pl.BlockSpec((pl.Element(rows), pl.Element(td)), tile),
            ]
            + [pl.BlockSpec((size, td), col) for size in (rows,) + tuple(s for s in sizes for _ in range(2))]
            + [any_spec] * n_prev,
            out_specs=[pl.BlockSpec((pl.Element(rows), pl.Element(td)), tile), any_spec],
            scratch_shapes=[
                pltpu.VMEM((rows, d_model), jnp.bfloat16),
                pltpu.VMEM((rows, d_hidden), jnp.bfloat16),
                pltpu.VMEM((rows, d_model), jnp.float32),
                pltpu.VMEM((rows, 128), jnp.float32),
                pltpu.VMEM((rows, d_model), jnp.bfloat16),
                pltpu.SemaphoreType.DMA,
                pltpu.SemaphoreType.DMA((rows // 128,)),
            ],
        ),
        out_shape=[out, out],
        input_output_aliases={} if previous is None else {n_fixed + 1 + 2 * len(sizes): 0, n_fixed + 1 + 2 * len(sizes) + 1: 1},
        compiler_params=pltpu.CompilerParams(vmem_limit_bytes=VMEM),
        cost_estimate=cost(rows, d_model, d_hidden),
    )(starts, x_in, w_gate, w_up, w_down, gain, residual, *received, *(previous or ()))


def solution(mesh):
    straight = [(p, (p + 2) % 4) for p in range(4)]
    crossed = [(p, (p + 2) % 4 ^ 1) for p in range(4)]
    partner_of = [(p, p ^ 1) for p in range(4)]

    def local_block(x_in, w_gate, w_up, w_down, residual, norm_gain):
        me = lax.axis_index("tp")
        weights = (x_in, w_gate, w_up, w_down)
        dest_a = ((me + 2) % 4) * 1024
        dest_b = ((me + 2) % 4 ^ 1) * 1024
        partner = (me ^ 1) * 1024

        def send(y, pairs):
            return lax.ppermute(y, "tp", pairs)

        recv = []
        at = 0
        y_a = x_in
        for half in CHUNKS:
            y_a, y_b = partial_rows((half, half), jnp.stack([dest_a + at, dest_b + at]), *weights, y_a)
            recv.append((send(y_a, straight), send(y_b, crossed)))
            at += half
        cut = CHUNKS[0] + CHUNKS[1]
        near = partial_rows((cut, 1024 - cut), jnp.stack([partner, partner + cut]), *weights, y_a)
        near = [send(y, partner_of) for y in near]
        gain = norm_gain.reshape(1, -1)
        outs = None
        for k, (row0, rows) in enumerate(((0, cut), (cut, 1024 - cut))):
            pieces = [near[k], *recv[2 * k], *recv[2 * k + 1]]
            start = jnp.stack([me * 1024 + row0])
            outs = own_rows(rows, row0, CHUNKS[2 * k : 2 * k + 2], start, *weights, gain, residual, pieces, outs)
        return tuple(outs)

    row_spec = P(("data", "tp"), None)
    return jax.shard_map(local_block, mesh=mesh, in_specs=(P("data", None), P(None, "tp"), P(None, "tp"), P("tp", None), row_spec, P(None)), out_specs=(row_spec, row_spec), check_vma=False)
```

```python
import functools

import jax
import jax.numpy as jnp
from jax import lax
from jax.experimental import pallas as pl
from jax.experimental.pallas import tpu as pltpu
from jax.sharding import PartitionSpec as P

EPS = 1e-5
TF = 384
TD = 512
HALVES = (192, 320, 512)
VMEM = 67043328
MESH = pl.DeviceIdType.MESH


def block_kernel(nf, nd, block, x_hbm, w_gate, w_up, w_down, residual, h_out, recv, stage, x, gate_buf, up_buf, down_buf, hidden, y_buf, in_buf, res_buf, h_buf, x_sem, gate_sem, up_sem, down_sem, stage_sem, send_sem, recv_sem, in_sem, res_sem, h_sem):
    me = lax.axis_index("tp")
    partner = me + 1 - 2 * lax.rem(me, 2)
    far = (lax.rem(me + 2, 4), lax.rem(partner + 2, 4))

    chunks = []
    at = 0
    for half in HALVES:
        chunks.append([(far[0], 0, at, half), (far[1], 1, at, half)])
        at += half
    chunks.append([(partner, 2, 0, block)])
    chunks.append([(me, 3, 0, block)])
    n_chunks = len(chunks)

    def x_copies(k):
        copies, row = [], 0
        for i, (owner, _, first, size) in enumerate(chunks[k]):
            src = x_hbm.at[pl.ds(pl.multiple_of(owner * block + first, 64), size)]
            copies.append(pltpu.make_async_copy(src, x.at[pl.ds(row, size)], x_sem.at[i]))
            row += size
        return copies

    def gate_copies(tile, slot):
        cols = pl.ds(pl.multiple_of(tile * TF, 128), TF)
        return [
            pltpu.make_async_copy(w_gate.at[:, cols], gate_buf.at[slot], gate_sem.at[slot]),
            pltpu.make_async_copy(w_up.at[:, cols], up_buf.at[slot], up_sem.at[slot]),
        ]

    def down_copy(tile, slot):
        cols = pl.ds(pl.multiple_of(tile * TD, 128), TD)
        return pltpu.make_async_copy(w_down.at[:, cols], down_buf.at[slot], down_sem.at[slot])

    def stage_copies(k, tile, slot):
        copies, row = [], 0
        for i, (_, src, first, size) in enumerate(chunks[k]):
            copies.append(pltpu.make_async_copy(y_buf.at[slot, pl.ds(row, size)], stage.at[tile, src, pl.ds(first, size)], stage_sem.at[slot, i]))
            row += size
        return copies

    def send_copies(k, tile):
        return [
            pltpu.make_async_remote_copy(
                src_ref=stage.at[tile, src, pl.ds(first, size)],
                dst_ref=recv.at[tile, src, pl.ds(first, size)],
                send_sem=send_sem,
                recv_sem=recv_sem.at[tile],
                device_id={"tp": owner},
                device_id_type=MESH,
            )
            for owner, src, first, size in chunks[k]
        ]

    def flush(k, tile, slot):
        for copy in stage_copies(k, tile, slot):
            copy.wait()
        for copy in send_copies(k, tile):
            copy.start()

    def in_copies(tile, slot):
        cols = pl.ds(pl.multiple_of(tile * TD, 128), TD)
        return [
            pltpu.make_async_copy(recv.at[tile], in_buf.at[slot], in_sem.at[slot]),
            pltpu.make_async_copy(residual.at[:, cols], res_buf.at[slot], res_sem.at[slot]),
        ]

    def h_copy(tile, slot):
        cols = pl.ds(pl.multiple_of(tile * TD, 128), TD)
        return pltpu.make_async_copy(h_buf.at[slot], h_out.at[:, cols], h_sem.at[slot])

    def fetch_in(tile, slot):
        pltpu.make_async_copy(recv.at[tile], recv.at[tile], recv_sem.at[tile]).wait()
        for copy in in_copies(tile, slot):
            copy.start()

    for copy in (*gate_copies(0, 0), *x_copies(0), *gate_copies(1, 1), down_copy(0, 0), down_copy(1, 1)):
        copy.start()
    barrier = pltpu.get_barrier_semaphore()
    for peer in (partner, *far):
        pl.semaphore_signal(barrier, inc=1, device_id={"tp": peer}, device_id_type=MESH)
    pl.semaphore_wait(barrier, 3)

    for k in range(n_chunks):
        rows = sum(size for _, _, _, size in chunks[k])
        last = k == n_chunks - 1
        for copy in x_copies(k):
            copy.wait()

        def gate_step(i, _, k=k, rows=rows):
            slot = lax.rem(k * nf + i, 2)
            for copy in gate_copies(i, slot):
                copy.wait()
            for piece in range(TF // 128):
                cols = slice(piece * 128, piece * 128 + 128)
                both = jnp.concatenate([gate_buf[slot, :, cols], up_buf[slot, :, cols]], axis=1)
                prod = jnp.dot(x[0:rows, :], both, preferred_element_type=jnp.float32)
                val = (jax.nn.silu(prod[:, :128]) * prod[:, 128:]).astype(jnp.bfloat16)
                hidden[0:rows, pl.ds(pl.multiple_of(i * TF + piece * 128, 128), 128)] = val
            if k == n_chunks - 1:

                @pl.when(i + 2 < nf)
                def _():
                    for copy in gate_copies(i + 2, slot):
                        copy.start()
            else:
                for copy in gate_copies(lax.rem(i + 2, nf), slot):
                    copy.start()
            return 0

        lax.fori_loop(0, nf, gate_step, 0)
        if k > 0:
            flush(k - 1, nd - 1, (nd - 1) % 2)
        if not last:
            for copy in x_copies(k + 1):
                copy.start()
        else:
            fetch_in(0, 0)

        def down_step(j, _, k=k, rows=rows, last=last):
            slot = lax.rem(j, 2)
            down_copy(j, slot).wait()
            prod = jnp.dot(hidden[0:rows, :], down_buf[slot], preferred_element_type=jnp.float32).astype(jnp.bfloat16)
            if not last:
                y_buf[slot, 0:rows] = prod

                @pl.when(j > 0)
                def _():
                    flush(k, j - 1, 1 - slot)

                for copy in stage_copies(k, j, slot):
                    copy.start()
                down_copy(lax.rem(j + 2, nd), slot).start()
            else:
                for copy in in_copies(j, slot):
                    copy.wait()

                @pl.when(j >= 2)
                def _():
                    h_copy(j - 2, slot).wait()

                total = prod.astype(jnp.float32) + in_buf[slot, 0].astype(jnp.float32)
                total = total + in_buf[slot, 1].astype(jnp.float32) + in_buf[slot, 2].astype(jnp.float32)
                h_buf[slot] = res_buf[slot].astype(jnp.float32) + total
                h_copy(j, slot).start()

                @pl.when(j + 2 < nd)
                def _():
                    down_copy(j + 2, slot).start()

                @pl.when(j + 1 < nd)
                def _():
                    fetch_in(j + 1, 1 - slot)

            return 0

        lax.fori_loop(0, nd, down_step, 0)

    for tile in (nd - 2, nd - 1):
        h_copy(tile, tile % 2).wait()
    pltpu.make_async_copy(stage, stage, send_sem).wait()


def block_sum(x_in, w_gate, w_up, w_down, residual):
    d_model, d_hidden = w_gate.shape
    block = residual.shape[0]
    rows = block
    nf, nd = d_hidden // TF, d_model // TD
    any_spec = pl.BlockSpec(memory_space=pl.ANY)
    bf16, f32 = jnp.bfloat16, jnp.float32
    dma = pltpu.SemaphoreType.DMA
    return pl.pallas_call(
        functools.partial(block_kernel, nf, nd, block),
        in_specs=[any_spec] * 5,
        out_specs=[any_spec] * 3,
        out_shape=[
            jax.ShapeDtypeStruct((block, d_model), f32),
            jax.ShapeDtypeStruct((nd, 3, block, TD), bf16),
            jax.ShapeDtypeStruct((nd, 3, block, TD), bf16),
        ],
        scratch_shapes=[
            pltpu.VMEM((rows, d_model), bf16),
            pltpu.VMEM((2, d_model, TF), bf16),
            pltpu.VMEM((2, d_model, TF), bf16),
            pltpu.VMEM((2, d_hidden, TD), bf16),
            pltpu.VMEM((rows, d_hidden), bf16),
            pltpu.VMEM((2, rows, TD), bf16),
            pltpu.VMEM((2, 3, block, TD), bf16),
            pltpu.VMEM((2, block, TD), bf16),
            pltpu.VMEM((2, block, TD), f32),
            dma((2,)),
            dma((2,)),
            dma((2,)),
            dma((2,)),
            dma((2, 2)),
            dma,
            dma((nd,)),
            dma((2,)),
            dma((2,)),
            dma((2,)),
        ],
        compiler_params=pltpu.CompilerParams(vmem_limit_bytes=VMEM, collective_id=0, has_side_effects=True),
        cost_estimate=pl.CostEstimate(flops=24 * block * d_model * d_hidden, bytes_accessed=36 * d_model * d_hidden, transcendentals=0),
        name="block_sum",
    )(x_in, w_gate, w_up, w_down, residual)[0]


def norm_kernel(h_ref, gain, h_out, n_out):
    h = h_ref[...]
    mean_sq = jnp.mean(h * h, axis=-1, keepdims=True)
    h_out[...] = h.astype(jnp.bfloat16)
    n_out[...] = (h * lax.rsqrt(mean_sq + EPS) * gain[...]).astype(jnp.bfloat16)


def norm_rows(h, gain):
    block, d_model = h.shape
    rows = 128
    spec = pl.BlockSpec((rows, d_model), lambda i: (i, 0))
    out = jax.ShapeDtypeStruct(h.shape, jnp.bfloat16)
    return pl.pallas_call(
        norm_kernel,
        grid=(block // rows,),
        in_specs=[spec, pl.BlockSpec((1, d_model), lambda i: (0, 0))],
        out_specs=[spec, spec],
        out_shape=[out, out],
        cost_estimate=pl.CostEstimate(flops=5 * block * d_model, bytes_accessed=8 * block * d_model, transcendentals=block),
        name="norm_rows",
    )(h, gain)


def solution(mesh):
    def local_block(x_in, w_gate, w_up, w_down, residual, norm_gain):
        h = block_sum(x_in, w_gate, w_up, w_down, residual)
        return tuple(norm_rows(h, norm_gain.reshape(1, -1)))

    row_spec = P(("data", "tp"), None)
    return jax.shard_map(local_block, mesh=mesh, in_specs=(P("data", None), P(None, "tp"), P(None, "tp"), P("tp", None), row_spec, P(None)), out_specs=(row_spec, row_spec), check_vma=False)
```

```python
import functools

import jax
import jax.numpy as jnp
from jax import lax
from jax.experimental import pallas as pl
from jax.experimental.pallas import tpu as pltpu
from jax.sharding import PartitionSpec as P

EPS = 1e-5
TF = 384
TD = 512
HALVES = (160, 320, 544)
VMEM = 67043328
MESH = pl.DeviceIdType.MESH


def block_kernel(nf, nd, block, x_hbm, w_gate, w_up, w_down, residual, h_out, sq_out, recv, stage, x, gate_buf, up_buf, down_buf, hidden, y_buf, in_buf, res_buf, h_buf, sq_buf, x_sem, gate_sem, up_sem, down_sem, stage_sem, send_sem, recv_sem, in_sem, res_sem, h_sem, sq_sem):
    me = lax.axis_index("tp")
    partner = me + 1 - 2 * lax.rem(me, 2)
    far = (lax.rem(me + 2, 4), lax.rem(partner + 2, 4))

    chunks = []
    at = 0
    for half in HALVES:
        chunks.append([(far[0], 0, at, half), (far[1], 1, at, half)])
        at += half
    chunks.append([(partner, 2, 0, block)])
    chunks.append([(me, 3, 0, block)])
    n_chunks = len(chunks)

    def x_copies(k):
        copies, row = [], 0
        for i, (owner, _, first, size) in enumerate(chunks[k]):
            src = x_hbm.at[pl.ds(pl.multiple_of(owner * block + first, 32), size)]
            copies.append(pltpu.make_async_copy(src, x.at[pl.ds(row, size)], x_sem.at[i]))
            row += size
        return copies

    def gate_copies(tile, slot):
        cols = pl.ds(pl.multiple_of(tile * TF, 128), TF)
        return [
            pltpu.make_async_copy(w_gate.at[:, cols], gate_buf.at[slot], gate_sem.at[slot]),
            pltpu.make_async_copy(w_up.at[:, cols], up_buf.at[slot], up_sem.at[slot]),
        ]

    def down_copy(tile, slot):
        cols = pl.ds(pl.multiple_of(tile * TD, 128), TD)
        return pltpu.make_async_copy(w_down.at[:, cols], down_buf.at[slot], down_sem.at[slot])

    def stage_copies(k, tile, slot):
        copies, row = [], 0
        for i, (_, src, first, size) in enumerate(chunks[k]):
            copies.append(pltpu.make_async_copy(y_buf.at[slot, pl.ds(row, size)], stage.at[tile, src, pl.ds(first, size)], stage_sem.at[slot, i]))
            row += size
        return copies

    def send_copies(k, tile):
        return [
            pltpu.make_async_remote_copy(
                src_ref=stage.at[tile, src, pl.ds(first, size)],
                dst_ref=recv.at[tile, src, pl.ds(first, size)],
                send_sem=send_sem,
                recv_sem=recv_sem.at[tile],
                device_id={"tp": owner},
                device_id_type=MESH,
            )
            for owner, src, first, size in chunks[k]
        ]

    def flush(k, tile, slot):
        for copy in stage_copies(k, tile, slot):
            copy.wait()
        for copy in send_copies(k, tile):
            copy.start()

    def in_copies(tile, slot):
        cols = pl.ds(pl.multiple_of(tile * TD, 128), TD)
        return [
            pltpu.make_async_copy(recv.at[tile], in_buf.at[slot], in_sem.at[slot]),
            pltpu.make_async_copy(residual.at[:, cols], res_buf.at[slot], res_sem.at[slot]),
        ]

    def h_copy(tile, slot):
        cols = pl.ds(pl.multiple_of(tile * TD, 128), TD)
        return pltpu.make_async_copy(h_buf.at[slot], h_out.at[:, cols], h_sem.at[slot])

    def fetch_in(tile, slot):
        pltpu.make_async_copy(recv.at[tile], recv.at[tile], recv_sem.at[tile]).wait()
        for copy in in_copies(tile, slot):
            copy.start()

    for copy in (*x_copies(0), *gate_copies(0, 0), *gate_copies(1, 1)):
        copy.start()
    barrier = pltpu.get_barrier_semaphore()
    for peer in (partner, *far):
        pl.semaphore_signal(barrier, inc=1, device_id={"tp": peer}, device_id_type=MESH)
    pl.semaphore_wait(barrier, 3)

    for k in range(n_chunks):
        rows = sum(size for _, _, _, size in chunks[k])
        last = k == n_chunks - 1
        for copy in x_copies(k):
            copy.wait()

        def gate_step(i, _, k=k, rows=rows):
            slot = lax.rem(k * nf + i, 2)
            for copy in gate_copies(i, slot):
                copy.wait()
            for piece in range(TF // 128):
                cols = slice(piece * 128, piece * 128 + 128)
                both = jnp.concatenate([gate_buf[slot, :, cols], up_buf[slot, :, cols]], axis=1)
                prod = jnp.dot(x[0:rows, :], both, preferred_element_type=jnp.float32)
                val = (jax.nn.silu(prod[:, :128]) * prod[:, 128:]).astype(jnp.bfloat16)
                hidden[0:rows, pl.ds(pl.multiple_of(i * TF + piece * 128, 128), 128)] = val
            if k == n_chunks - 1:

                @pl.when(i + 2 < nf)
                def _():
                    for copy in gate_copies(i + 2, slot):
                        copy.start()
            else:
                for copy in gate_copies(lax.rem(i + 2, nf), slot):
                    copy.start()
            return 0

        if k == 0:
            lax.fori_loop(0, nf - 3, gate_step, 0)
            for tile in (0, 1):
                down_copy(tile, tile).start()
            lax.fori_loop(nf - 3, nf, gate_step, 0)
        else:
            lax.fori_loop(0, nf, gate_step, 0)
        if k > 0:
            flush(k - 1, nd - 1, (nd - 1) % 2)
        if not last:
            for copy in x_copies(k + 1):
                copy.start()
        else:
            fetch_in(0, 0)

        if last:
            break

        def down_step(j, _, k=k, rows=rows):
            slot = lax.rem(j, 2)
            down_copy(j, slot).wait()
            y_buf[slot, 0:rows] = jnp.dot(hidden[0:rows, :], down_buf[slot], preferred_element_type=jnp.float32).astype(jnp.bfloat16)

            @pl.when(j > 0)
            def _():
                flush(k, j - 1, 1 - slot)

            for copy in stage_copies(k, j, slot):
                copy.start()
            down_copy(lax.rem(j + 2, nd), slot).start()
            return 0

        lax.fori_loop(0, nd, down_step, 0)

    def own_dot(slot):
        y_buf[slot, 0:block] = jnp.dot(hidden[0:block, :], down_buf[slot], preferred_element_type=jnp.float32).astype(jnp.bfloat16)

    def combine(slot):
        total = y_buf[slot, 0:block].astype(jnp.float32) + in_buf[slot, 2].astype(jnp.float32)
        total = total + in_buf[slot, 0].astype(jnp.float32) + in_buf[slot, 1].astype(jnp.float32)
        h = res_buf[slot].astype(jnp.float32) + total
        h_buf[slot] = h
        sq = h * h
        acc = sq_buf[...]
        for c in range(TD // 128):
            acc = acc + sq[:, c * 128 : c * 128 + 128]
        sq_buf[...] = acc

    sq_buf[...] = jnp.zeros_like(sq_buf)
    down_copy(0, 0).wait()
    own_dot(0)
    down_copy(2, 0).start()

    def own_step(j, _):
        slot = lax.rem(j, 2)
        down_copy(j, slot).wait()
        for copy in in_copies(j - 1, 1 - slot):
            copy.wait()

        @pl.when(j >= 3)
        def _():
            h_copy(j - 3, 1 - slot).wait()

        combine(1 - slot)
        own_dot(slot)
        h_copy(j - 1, 1 - slot).start()

        @pl.when(j + 2 < nd)
        def _():
            down_copy(j + 2, slot).start()

        fetch_in(j, slot)
        return 0

    lax.fori_loop(1, nd, own_step, 0)
    end = (nd - 1) % 2
    for copy in in_copies(nd - 1, end):
        copy.wait()
    h_copy(nd - 3, end).wait()
    combine(end)
    h_copy(nd - 1, end).start()
    sq_copy = pltpu.make_async_copy(sq_buf, sq_out, sq_sem)
    sq_copy.start()
    h_copy(nd - 2, 1 - end).wait()
    h_copy(nd - 1, end).wait()
    sq_copy.wait()
    pltpu.make_async_copy(stage, stage, send_sem).wait()


def block_sum(x_in, w_gate, w_up, w_down, residual):
    d_model, d_hidden = w_gate.shape
    block = residual.shape[0]
    rows = max(block, 2 * max(HALVES))
    nf, nd = d_hidden // TF, d_model // TD
    any_spec = pl.BlockSpec(memory_space=pl.ANY)
    bf16, f32 = jnp.bfloat16, jnp.float32
    dma = pltpu.SemaphoreType.DMA
    return pl.pallas_call(
        functools.partial(block_kernel, nf, nd, block),
        in_specs=[any_spec] * 5,
        out_specs=[any_spec] * 4,
        out_shape=[
            jax.ShapeDtypeStruct((block, d_model), f32),
            jax.ShapeDtypeStruct((block, 128), f32),
            jax.ShapeDtypeStruct((nd, 3, block, TD), bf16),
            jax.ShapeDtypeStruct((nd, 3, block, TD), bf16),
        ],
        scratch_shapes=[
            pltpu.VMEM((rows, d_model), bf16),
            pltpu.VMEM((2, d_model, TF), bf16),
            pltpu.VMEM((2, d_model, TF), bf16),
            pltpu.VMEM((2, d_hidden, TD), bf16),
            pltpu.VMEM((rows, d_hidden), bf16),
            pltpu.VMEM((2, rows, TD), bf16),
            pltpu.VMEM((2, 3, block, TD), bf16),
            pltpu.VMEM((2, block, TD), bf16),
            pltpu.VMEM((2, block, TD), f32),
            pltpu.VMEM((block, 128), f32),
            dma((2,)),
            dma((2,)),
            dma((2,)),
            dma((2,)),
            dma((2, 2)),
            dma,
            dma((nd,)),
            dma((2,)),
            dma((2,)),
            dma((2,)),
            dma,
        ],
        compiler_params=pltpu.CompilerParams(vmem_limit_bytes=VMEM, collective_id=0, has_side_effects=True),
        cost_estimate=pl.CostEstimate(flops=24 * block * d_model * d_hidden, bytes_accessed=36 * d_model * d_hidden, transcendentals=0),
        name="block_sum",
    )(x_in, w_gate, w_up, w_down, residual)[:2]


def norm_kernel(h_ref, sq, gain, h_out, n_out):
    d_model = h_ref.shape[1]
    h = h_ref[...]
    scale = lax.rsqrt(jnp.sum(sq[...], axis=1, keepdims=True) / d_model + EPS)
    h_out[...] = h.astype(jnp.bfloat16)
    n_out[...] = (h * scale * gain[...]).astype(jnp.bfloat16)


def norm_rows(h, sq, gain):
    block, d_model = h.shape
    rows = 128
    spec = pl.BlockSpec((rows, d_model), lambda i: (i, 0))
    out = jax.ShapeDtypeStruct(h.shape, jnp.bfloat16)
    return pl.pallas_call(
        norm_kernel,
        grid=(block // rows,),
        in_specs=[spec, pl.BlockSpec((rows, 128), lambda i: (i, 0)), pl.BlockSpec((1, d_model), lambda i: (0, 0))],
        out_specs=[spec, spec],
        out_shape=[out, out],
        cost_estimate=pl.CostEstimate(flops=5 * block * d_model, bytes_accessed=8 * block * d_model, transcendentals=block),
        name="norm_rows",
    )(h, sq, gain)


def solution(mesh):
    def local_block(x_in, w_gate, w_up, w_down, residual, norm_gain):
        h, sq = block_sum(x_in, w_gate, w_up, w_down, residual)
        return tuple(norm_rows(h, sq, norm_gain.reshape(1, -1)))

    row_spec = P(("data", "tp"), None)
    return jax.shard_map(local_block, mesh=mesh, in_specs=(P("data", None), P(None, "tp"), P(None, "tp"), P("tp", None), row_spec, P(None)), out_specs=(row_spec, row_spec), check_vma=False)
```

```python
import functools

import jax
import jax.numpy as jnp
from jax import lax
from jax.experimental import pallas as pl
from jax.experimental.pallas import tpu as pltpu
from jax.sharding import PartitionSpec as P

EPS = 1e-5
TF = 384
TD = 512
HALVES = (160, 352, 512)
VMEM = 67043328
MESH = pl.DeviceIdType.MESH


def block_kernel(nf, nd, block, x_hbm, w_gate, w_up, w_down, residual, h_out, sq_out, recv, stage, x, gate_buf, up_buf, down_buf, hidden, y_buf, in_buf, res_buf, h_buf, sq_buf, x_sem, gate_sem, up_sem, down_sem, stage_sem, send_sem, recv_sem, in_sem, res_sem, h_sem, sq_sem):
    me = lax.axis_index("tp")
    partner = me + 1 - 2 * lax.rem(me, 2)
    far = (lax.rem(me + 2, 4), lax.rem(partner + 2, 4))

    chunks = []
    at = 0
    for half in HALVES:
        chunks.append([(far[0], 0, at, half), (far[1], 1, at, half)])
        at += half
    chunks.append([(partner, 2, 0, block)])
    chunks.append([(me, 3, 0, block)])
    n_chunks = len(chunks)

    def x_copies(k):
        copies, row = [], 0
        for i, (owner, _, first, size) in enumerate(chunks[k]):
            src = x_hbm.at[pl.ds(pl.multiple_of(owner * block + first, 32), size)]
            copies.append(pltpu.make_async_copy(src, x.at[pl.ds(row, size)], x_sem.at[i]))
            row += size
        return copies

    def gate_copies(tile, slot):
        cols = pl.ds(pl.multiple_of(tile * TF, 128), TF)
        return [
            pltpu.make_async_copy(w_gate.at[:, cols], gate_buf.at[slot], gate_sem.at[slot]),
            pltpu.make_async_copy(w_up.at[:, cols], up_buf.at[slot], up_sem.at[slot]),
        ]

    def down_copy(tile, slot):
        cols = pl.ds(pl.multiple_of(tile * TD, 128), TD)
        return pltpu.make_async_copy(w_down.at[:, cols], down_buf.at[slot], down_sem.at[slot])

    def stage_copies(k, tile, slot):
        copies, row = [], 0
        for i, (_, src, first, size) in enumerate(chunks[k]):
            copies.append(pltpu.make_async_copy(y_buf.at[slot, pl.ds(row, size)], stage.at[tile, src, pl.ds(first, size)], stage_sem.at[slot, i]))
            row += size
        return copies

    def send_copies(k, tile):
        return [
            pltpu.make_async_remote_copy(
                src_ref=stage.at[tile, src, pl.ds(first, size)],
                dst_ref=recv.at[tile, src, pl.ds(first, size)],
                send_sem=send_sem,
                recv_sem=recv_sem.at[tile],
                device_id={"tp": owner},
                device_id_type=MESH,
            )
            for owner, src, first, size in chunks[k]
        ]

    def flush(k, tile, slot):
        for copy in stage_copies(k, tile, slot):
            copy.wait()
        for copy in send_copies(k, tile):
            copy.start()

    def in_copies(tile, slot):
        cols = pl.ds(pl.multiple_of(tile * TD, 128), TD)
        return [
            pltpu.make_async_copy(recv.at[tile], in_buf.at[slot], in_sem.at[slot]),
            pltpu.make_async_copy(residual.at[:, cols], res_buf.at[slot], res_sem.at[slot]),
        ]

    def h_copy(tile, slot):
        cols = pl.ds(pl.multiple_of(tile * TD, 128), TD)
        return pltpu.make_async_copy(h_buf.at[slot], h_out.at[:, cols], h_sem.at[slot])

    def fetch_in(tile, slot):
        pltpu.make_async_copy(recv.at[tile], recv.at[tile], recv_sem.at[tile]).wait()
        for copy in in_copies(tile, slot):
            copy.start()

    for copy in (*x_copies(0), *gate_copies(0, 0), *gate_copies(1, 1)):
        copy.start()
    barrier = pltpu.get_barrier_semaphore()
    for peer in (partner, *far):
        pl.semaphore_signal(barrier, inc=1, device_id={"tp": peer}, device_id_type=MESH)
    pl.semaphore_wait(barrier, 3)

    for k in range(n_chunks):
        rows = sum(size for _, _, _, size in chunks[k])
        last = k == n_chunks - 1
        for copy in x_copies(k):
            copy.wait()

        def gate_step(i, _, k=k, rows=rows):
            slot = lax.rem(k * nf + i, 2)
            for copy in gate_copies(i, slot):
                copy.wait()
            for piece in range(TF // 128):
                cols = slice(piece * 128, piece * 128 + 128)
                both = jnp.concatenate([gate_buf[slot, :, cols], up_buf[slot, :, cols]], axis=1)
                prod = jnp.dot(x[0:rows, :], both, preferred_element_type=jnp.float32)
                val = (jax.nn.silu(prod[:, :128]) * prod[:, 128:]).astype(jnp.bfloat16)
                hidden[0:rows, pl.ds(pl.multiple_of(i * TF + piece * 128, 128), 128)] = val
            if k == 0:

                @pl.when(i == nf - 4)
                def _():
                    for tile in (0, 1):
                        down_copy(tile, tile).start()
            else:

                @pl.when(i == 0)
                def _():
                    flush(k - 1, nd - 1, (nd - 1) % 2)

            if k == n_chunks - 1:

                @pl.when(i + 2 < nf)
                def _():
                    for copy in gate_copies(i + 2, slot):
                        copy.start()
            else:
                for copy in gate_copies(lax.rem(i + 2, nf), slot):
                    copy.start()
            return 0

        lax.fori_loop(0, nf, gate_step, 0)
        if not last:
            for copy in x_copies(k + 1):
                copy.start()
        else:
            fetch_in(0, 0)

        if last:
            break

        def down_step(j, _, k=k, rows=rows):
            slot = lax.rem(j, 2)
            down_copy(j, slot).wait()
            y_buf[slot, 0:rows] = jnp.dot(hidden[0:rows, :], down_buf[slot], preferred_element_type=jnp.float32).astype(jnp.bfloat16)

            @pl.when(j > 0)
            def _():
                flush(k, j - 1, 1 - slot)

            for copy in stage_copies(k, j, slot):
                copy.start()
            down_copy(lax.rem(j + 2, nd), slot).start()
            return 0

        lax.fori_loop(0, nd, down_step, 0)

    def own_dot(slot):
        y_buf[slot, 0:block] = jnp.dot(hidden[0:block, :], down_buf[slot], preferred_element_type=jnp.float32).astype(jnp.bfloat16)

    def combine(slot):
        total = y_buf[slot, 0:block].astype(jnp.float32) + in_buf[slot, 2].astype(jnp.float32)
        total = total + in_buf[slot, 0].astype(jnp.float32) + in_buf[slot, 1].astype(jnp.float32)
        h = res_buf[slot].astype(jnp.float32) + total
        h_buf[slot] = h
        sq = h * h
        acc = sq_buf[...]
        for c in range(TD // 128):
            acc = acc + sq[:, c * 128 : c * 128 + 128]
        sq_buf[...] = acc

    sq_buf[...] = jnp.zeros_like(sq_buf)
    down_copy(0, 0).wait()
    own_dot(0)
    down_copy(2, 0).start()

    def own_step(j, _):
        slot = lax.rem(j, 2)
        down_copy(j, slot).wait()
        for copy in in_copies(j - 1, 1 - slot):
            copy.wait()

        @pl.when(j >= 3)
        def _():
            h_copy(j - 3, 1 - slot).wait()

        combine(1 - slot)
        own_dot(slot)
        h_copy(j - 1, 1 - slot).start()

        @pl.when(j + 2 < nd)
        def _():
            down_copy(j + 2, slot).start()

        fetch_in(j, slot)
        return 0

    lax.fori_loop(1, nd, own_step, 0)
    end = (nd - 1) % 2
    for copy in in_copies(nd - 1, end):
        copy.wait()
    h_copy(nd - 3, end).wait()
    combine(end)
    h_copy(nd - 1, end).start()
    sq_copy = pltpu.make_async_copy(sq_buf, sq_out, sq_sem)
    sq_copy.start()
    h_copy(nd - 2, 1 - end).wait()
    h_copy(nd - 1, end).wait()
    sq_copy.wait()
    pltpu.make_async_copy(stage, stage, send_sem).wait()


def block_sum(x_in, w_gate, w_up, w_down, residual):
    d_model, d_hidden = w_gate.shape
    block = residual.shape[0]
    rows = max(block, 2 * max(HALVES))
    nf, nd = d_hidden // TF, d_model // TD
    any_spec = pl.BlockSpec(memory_space=pl.ANY)
    bf16, f32 = jnp.bfloat16, jnp.float32
    dma = pltpu.SemaphoreType.DMA
    return pl.pallas_call(
        functools.partial(block_kernel, nf, nd, block),
        in_specs=[any_spec] * 5,
        out_specs=[any_spec] * 4,
        out_shape=[
            jax.ShapeDtypeStruct((block, d_model), f32),
            jax.ShapeDtypeStruct((block, 128), f32),
            jax.ShapeDtypeStruct((nd, 3, block, TD), bf16),
            jax.ShapeDtypeStruct((nd, 3, block, TD), bf16),
        ],
        scratch_shapes=[
            pltpu.VMEM((rows, d_model), bf16),
            pltpu.VMEM((2, d_model, TF), bf16),
            pltpu.VMEM((2, d_model, TF), bf16),
            pltpu.VMEM((2, d_hidden, TD), bf16),
            pltpu.VMEM((rows, d_hidden), bf16),
            pltpu.VMEM((2, rows, TD), bf16),
            pltpu.VMEM((2, 3, block, TD), bf16),
            pltpu.VMEM((2, block, TD), bf16),
            pltpu.VMEM((2, block, TD), f32),
            pltpu.VMEM((block, 128), f32),
            dma((2,)),
            dma((2,)),
            dma((2,)),
            dma((2,)),
            dma((2, 2)),
            dma,
            dma((nd,)),
            dma((2,)),
            dma((2,)),
            dma((2,)),
            dma,
        ],
        compiler_params=pltpu.CompilerParams(vmem_limit_bytes=VMEM, collective_id=0, has_side_effects=True),
        cost_estimate=pl.CostEstimate(flops=24 * block * d_model * d_hidden, bytes_accessed=36 * d_model * d_hidden, transcendentals=0),
        name="block_sum",
    )(x_in, w_gate, w_up, w_down, residual)[:2]


def norm_kernel(h_ref, sq, gain, h_out, n_out):
    d_model = h_ref.shape[1]
    h = h_ref[...]
    scale = lax.rsqrt(jnp.sum(sq[...], axis=1, keepdims=True) / d_model + EPS)
    h_out[...] = h.astype(jnp.bfloat16)
    n_out[...] = (h * scale * gain[...]).astype(jnp.bfloat16)


def norm_rows(h, sq, gain):
    block, d_model = h.shape
    rows = 128
    spec = pl.BlockSpec((rows, d_model), lambda i: (i, 0))
    out = jax.ShapeDtypeStruct(h.shape, jnp.bfloat16)
    return pl.pallas_call(
        norm_kernel,
        grid=(block // rows,),
        in_specs=[spec, pl.BlockSpec((rows, 128), lambda i: (i, 0)), pl.BlockSpec((1, d_model), lambda i: (0, 0))],
        out_specs=[spec, spec],
        out_shape=[out, out],
        cost_estimate=pl.CostEstimate(flops=5 * block * d_model, bytes_accessed=8 * block * d_model, transcendentals=block),
        name="norm_rows",
    )(h, sq, gain)


def solution(mesh):
    def local_block(x_in, w_gate, w_up, w_down, residual, norm_gain):
        h, sq = block_sum(x_in, w_gate, w_up, w_down, residual)
        return tuple(norm_rows(h, sq, norm_gain.reshape(1, -1)))

    row_spec = P(("data", "tp"), None)
    return jax.shard_map(local_block, mesh=mesh, in_specs=(P("data", None), P(None, "tp"), P(None, "tp"), P("tp", None), row_spec, P(None)), out_specs=(row_spec, row_spec), check_vma=False)
```

```python
import functools

import jax
import jax.numpy as jnp
from jax import lax
from jax.experimental import pallas as pl
from jax.experimental.pallas import tpu as pltpu
from jax.sharding import PartitionSpec as P

EPS = 1e-5
TF = 384
TD = 512
HALVES = (160, 352, 512)
VMEM = 67043328
MESH = pl.DeviceIdType.MESH


def block_kernel(nf, nd, block, x_hbm, w_gate, w_up, w_down, residual, h_out, sq_out, recv, stage, x, gate_buf, up_buf, down_buf, hidden, y_buf, in_buf, res_buf, h_buf, sq_buf, x_sem, gate_sem, up_sem, down_sem, stage_sem, send_sem, recv_sem, in_sem, res_sem, h_sem, sq_sem):
    me = lax.axis_index("tp")
    partner = me + 1 - 2 * lax.rem(me, 2)
    far = (lax.rem(me + 2, 4), lax.rem(partner + 2, 4))

    chunks = []
    at = 0
    for half in HALVES:
        chunks.append([(far[0], 0, at, half), (far[1], 1, at, half)])
        at += half
    chunks.append([(partner, 2, 0, block)])
    chunks.append([(me, 3, 0, block)])
    n_chunks = len(chunks)

    def x_copies(k):
        copies, row = [], 0
        for i, (owner, _, first, size) in enumerate(chunks[k]):
            src = x_hbm.at[pl.ds(pl.multiple_of(owner * block + first, 32), size)]
            copies.append(pltpu.make_async_copy(src, x.at[pl.ds(row, size)], x_sem.at[i]))
            row += size
        return copies

    def gate_copies(tile, slot):
        cols = pl.ds(pl.multiple_of(tile * TF, 128), TF)
        return [
            pltpu.make_async_copy(w_gate.at[:, cols], gate_buf.at[slot], gate_sem.at[slot]),
            pltpu.make_async_copy(w_up.at[:, cols], up_buf.at[slot], up_sem.at[slot]),
        ]

    def down_copy(tile, slot):
        cols = pl.ds(pl.multiple_of(tile * TD, 128), TD)
        return pltpu.make_async_copy(w_down.at[:, cols], down_buf.at[slot], down_sem.at[slot])

    def stage_copies(k, tile, slot):
        copies, row = [], 0
        for i, (_, src, first, size) in enumerate(chunks[k]):
            copies.append(pltpu.make_async_copy(y_buf.at[slot, pl.ds(row, size)], stage.at[tile, src, pl.ds(first, size)], stage_sem.at[slot, i]))
            row += size
        return copies

    def send_copies(k, tile):
        return [
            pltpu.make_async_remote_copy(
                src_ref=stage.at[tile, src, pl.ds(first, size)],
                dst_ref=recv.at[tile, src, pl.ds(first, size)],
                send_sem=send_sem,
                recv_sem=recv_sem.at[tile],
                device_id={"tp": owner},
                device_id_type=MESH,
            )
            for owner, src, first, size in chunks[k]
        ]

    def flush(k, tile, slot):
        for copy in stage_copies(k, tile, slot):
            copy.wait()
        for copy in send_copies(k, tile):
            copy.start()

    def in_copies(tile, slot):
        cols = pl.ds(pl.multiple_of(tile * TD, 128), TD)
        return [
            pltpu.make_async_copy(recv.at[tile], in_buf.at[slot], in_sem.at[slot]),
            pltpu.make_async_copy(residual.at[:, cols], res_buf.at[slot], res_sem.at[slot]),
        ]

    def h_copy(tile, slot):
        cols = pl.ds(pl.multiple_of(tile * TD, 128), TD)
        return pltpu.make_async_copy(h_buf.at[slot], h_out.at[:, cols], h_sem.at[slot])

    def fetch_in(tile, slot):
        pltpu.make_async_copy(recv.at[tile], recv.at[tile], recv_sem.at[tile]).wait()
        for copy in in_copies(tile, slot):
            copy.start()

    for copy in (*x_copies(0), *gate_copies(0, 0), *gate_copies(1, 1)):
        copy.start()
    barrier = pltpu.get_barrier_semaphore()
    for peer in (partner, *far):
        pl.semaphore_signal(barrier, inc=1, device_id={"tp": peer}, device_id_type=MESH)
    pl.semaphore_wait(barrier, 3)

    for k in range(n_chunks):
        rows = sum(size for _, _, _, size in chunks[k])
        last = k == n_chunks - 1
        for copy in x_copies(k):
            copy.wait()

        def gate_step(i, _, k=k, rows=rows):
            slot = lax.rem(k * nf + i, 2)
            for copy in gate_copies(i, slot):
                copy.wait()
            for piece in range(TF // 128):
                cols = slice(piece * 128, piece * 128 + 128)
                both = jnp.concatenate([gate_buf[slot, :, cols], up_buf[slot, :, cols]], axis=1)
                prod = jnp.dot(x[0:rows, :], both, preferred_element_type=jnp.float32)
                val = (jax.nn.silu(prod[:, :128]) * prod[:, 128:]).astype(jnp.bfloat16)
                hidden[0:rows, pl.ds(pl.multiple_of(i * TF + piece * 128, 128), 128)] = val
            if k == 0:

                @pl.when(i == nf - 4)
                def _():
                    for tile in (0, 1):
                        down_copy(tile, tile).start()
            else:

                @pl.when(i == 0)
                def _():
                    flush(k - 1, nd - 1, (nd - 1) % 2)

            if k == n_chunks - 1:

                @pl.when(i + 2 < nf)
                def _():
                    for copy in gate_copies(i + 2, slot):
                        copy.start()
            else:
                for copy in gate_copies(lax.rem(i + 2, nf), slot):
                    copy.start()
            return 0

        lax.fori_loop(0, nf, gate_step, 0)
        if not last:
            for copy in x_copies(k + 1):
                copy.start()
        else:
            fetch_in(0, 0)

        if last:
            break

        def down_step(j, _, k=k, rows=rows):
            slot = lax.rem(j, 2)
            down_copy(j, slot).wait()
            y_buf[slot, 0:rows] = jnp.dot(hidden[0:rows, :], down_buf[slot], preferred_element_type=jnp.float32).astype(jnp.bfloat16)

            @pl.when(j > 0)
            def _():
                flush(k, j - 1, 1 - slot)

            for copy in stage_copies(k, j, slot):
                copy.start()
            down_copy(lax.rem(j + 2, nd), slot).start()
            return 0

        lax.fori_loop(0, nd, down_step, 0)

    def own_dot(slot):
        y_buf[slot, 0:block] = jnp.dot(hidden[0:block, :], down_buf[slot], preferred_element_type=jnp.float32).astype(jnp.bfloat16)

    def combine(slot):
        total = y_buf[slot, 0:block].astype(jnp.float32) + in_buf[slot, 2].astype(jnp.float32)
        total = total + in_buf[slot, 0].astype(jnp.float32) + in_buf[slot, 1].astype(jnp.float32)
        h = res_buf[slot].astype(jnp.float32) + total
        h_buf[slot] = h
        sq = h * h
        acc = sq_buf[...]
        for c in range(TD // 128):
            acc = acc + sq[:, c * 128 : c * 128 + 128]
        sq_buf[...] = acc

    sq_buf[...] = jnp.zeros_like(sq_buf)
    down_copy(0, 0).wait()
    own_dot(0)
    down_copy(2, 0).start()
    fetch_in(1, 1)

    def own_step(j, _):
        slot = lax.rem(j, 2)
        down_copy(j, slot).wait()
        for copy in in_copies(j - 1, 1 - slot):
            copy.wait()

        @pl.when(j >= 3)
        def _():
            h_copy(j - 3, 1 - slot).wait()

        combine(1 - slot)
        own_dot(slot)
        h_copy(j - 1, 1 - slot).start()

        @pl.when(j + 2 < nd)
        def _():
            down_copy(j + 2, slot).start()

        @pl.when(j + 2 < nd)
        def _():
            fetch_in(j + 1, 1 - slot)

        return 0

    lax.fori_loop(1, nd, own_step, 0)
    end = (nd - 1) % 2
    fetch_in(nd - 1, end)
    for copy in in_copies(nd - 1, end):
        copy.wait()
    h_copy(nd - 3, end).wait()
    combine(end)
    h_copy(nd - 1, end).start()
    sq_copy = pltpu.make_async_copy(sq_buf, sq_out, sq_sem)
    sq_copy.start()
    h_copy(nd - 2, 1 - end).wait()
    h_copy(nd - 1, end).wait()
    sq_copy.wait()
    pltpu.make_async_copy(stage, stage, send_sem).wait()


def block_sum(x_in, w_gate, w_up, w_down, residual):
    d_model, d_hidden = w_gate.shape
    block = residual.shape[0]
    rows = max(block, 2 * max(HALVES))
    nf, nd = d_hidden // TF, d_model // TD
    any_spec = pl.BlockSpec(memory_space=pl.ANY)
    bf16, f32 = jnp.bfloat16, jnp.float32
    dma = pltpu.SemaphoreType.DMA
    return pl.pallas_call(
        functools.partial(block_kernel, nf, nd, block),
        in_specs=[any_spec] * 5,
        out_specs=[any_spec] * 4,
        out_shape=[
            jax.ShapeDtypeStruct((block, d_model), f32),
            jax.ShapeDtypeStruct((block, 128), f32),
            jax.ShapeDtypeStruct((nd, 3, block, TD), bf16),
            jax.ShapeDtypeStruct((nd, 3, block, TD), bf16),
        ],
        scratch_shapes=[
            pltpu.VMEM((rows, d_model), bf16),
            pltpu.VMEM((2, d_model, TF), bf16),
            pltpu.VMEM((2, d_model, TF), bf16),
            pltpu.VMEM((2, d_hidden, TD), bf16),
            pltpu.VMEM((rows, d_hidden), bf16),
            pltpu.VMEM((2, rows, TD), bf16),
            pltpu.VMEM((2, 3, block, TD), bf16),
            pltpu.VMEM((2, block, TD), bf16),
            pltpu.VMEM((2, block, TD), f32),
            pltpu.VMEM((block, 128), f32),
            dma((2,)),
            dma((2,)),
            dma((2,)),
            dma((2,)),
            dma((2, 2)),
            dma,
            dma((nd,)),
            dma((2,)),
            dma((2,)),
            dma((2,)),
            dma,
        ],
        compiler_params=pltpu.CompilerParams(vmem_limit_bytes=VMEM, collective_id=0, has_side_effects=True),
        cost_estimate=pl.CostEstimate(flops=24 * block * d_model * d_hidden, bytes_accessed=36 * d_model * d_hidden, transcendentals=0),
        name="block_sum",
    )(x_in, w_gate, w_up, w_down, residual)[:2]


def norm_kernel(h_ref, sq, gain, h_out, n_out):
    d_model = h_ref.shape[1]
    h = h_ref[...]
    scale = lax.rsqrt(jnp.sum(sq[...], axis=1, keepdims=True) / d_model + EPS)
    h_out[...] = h.astype(jnp.bfloat16)
    n_out[...] = (h * scale * gain[...]).astype(jnp.bfloat16)


def norm_rows(h, sq, gain):
    block, d_model = h.shape
    rows = 128
    spec = pl.BlockSpec((rows, d_model), lambda i: (i, 0))
    out = jax.ShapeDtypeStruct(h.shape, jnp.bfloat16)
    return pl.pallas_call(
        norm_kernel,
        grid=(block // rows,),
        in_specs=[spec, pl.BlockSpec((rows, 128), lambda i: (i, 0)), pl.BlockSpec((1, d_model), lambda i: (0, 0))],
        out_specs=[spec, spec],
        out_shape=[out, out],
        cost_estimate=pl.CostEstimate(flops=5 * block * d_model, bytes_accessed=8 * block * d_model, transcendentals=block),
        name="norm_rows",
    )(h, sq, gain)


def solution(mesh):
    def local_block(x_in, w_gate, w_up, w_down, residual, norm_gain):
        h, sq = block_sum(x_in, w_gate, w_up, w_down, residual)
        return tuple(norm_rows(h, sq, norm_gain.reshape(1, -1)))

    row_spec = P(("data", "tp"), None)
    return jax.shard_map(local_block, mesh=mesh, in_specs=(P("data", None), P(None, "tp"), P(None, "tp"), P("tp", None), row_spec, P(None)), out_specs=(row_spec, row_spec), check_vma=False)
```

```python
import functools

import jax
import jax.numpy as jnp
from jax import lax
from jax.experimental import pallas as pl
from jax.experimental.pallas import tpu as pltpu
from jax.sharding import PartitionSpec as P

EPS = 1e-5
TF = 384
TD = 512
HALVES = (192, 320, 512)
VMEM = 67043328
MESH = pl.DeviceIdType.MESH


def block_kernel(nf, nd, block, x_hbm, w_gate, w_up, w_down, residual, h_out, sq_out, recv, stage, x, gate_buf, up_buf, down_buf, hidden, y_buf, in_buf, res_buf, h_buf, sq_buf, x_sem, gate_sem, up_sem, down_sem, stage_sem, send_sem, recv_sem, in_sem, res_sem, h_sem, sq_sem):
    me = lax.axis_index("tp")
    partner = me + 1 - 2 * lax.rem(me, 2)
    far = (lax.rem(me + 2, 4), lax.rem(partner + 2, 4))

    chunks = []
    at = 0
    for half in HALVES:
        chunks.append([(far[0], 0, at, half), (far[1], 1, at, half)])
        at += half
    chunks.append([(partner, 2, 0, block)])
    chunks.append([(me, 3, 0, block)])
    n_chunks = len(chunks)

    def x_copies(k):
        copies, row = [], 0
        for i, (owner, _, first, size) in enumerate(chunks[k]):
            src = x_hbm.at[pl.ds(pl.multiple_of(owner * block + first, 32), size)]
            copies.append(pltpu.make_async_copy(src, x.at[pl.ds(row, size)], x_sem.at[i]))
            row += size
        return copies

    def gate_copies(tile, slot):
        cols = pl.ds(pl.multiple_of(tile * TF, 128), TF)
        half = w_gate.shape[0] // 2
        copies = []
        for part in range(2):
            here = pl.ds(part * half, half)
            copies.append(pltpu.make_async_copy(w_gate.at[here, cols], gate_buf.at[slot, here], gate_sem.at[slot, part]))
            copies.append(pltpu.make_async_copy(w_up.at[here, cols], up_buf.at[slot, here], up_sem.at[slot, part]))
        return copies

    def down_copy(tile, slot):
        cols = pl.ds(pl.multiple_of(tile * TD, 128), TD)
        return pltpu.make_async_copy(w_down.at[:, cols], down_buf.at[slot], down_sem.at[slot])

    def stage_copies(k, tile, slot):
        copies, row = [], 0
        for i, (_, src, first, size) in enumerate(chunks[k]):
            copies.append(pltpu.make_async_copy(y_buf.at[slot, pl.ds(row, size)], stage.at[tile, src, pl.ds(first, size)], stage_sem.at[slot, i]))
            row += size
        return copies

    def send_copies(k, tile):
        return [
            pltpu.make_async_remote_copy(
                src_ref=stage.at[tile, src, pl.ds(first, size)],
                dst_ref=recv.at[tile, src, pl.ds(first, size)],
                send_sem=send_sem,
                recv_sem=recv_sem.at[tile],
                device_id={"tp": owner},
                device_id_type=MESH,
            )
            for owner, src, first, size in chunks[k]
        ]

    def flush(k, tile, slot):
        for copy in stage_copies(k, tile, slot):
            copy.wait()
        for copy in send_copies(k, tile):
            copy.start()

    def in_copies(tile, slot):
        cols = pl.ds(pl.multiple_of(tile * TD, 128), TD)
        return [
            pltpu.make_async_copy(recv.at[tile], in_buf.at[slot], in_sem.at[slot]),
            pltpu.make_async_copy(residual.at[:, cols], res_buf.at[slot], res_sem.at[slot]),
        ]

    def h_copy(tile, slot):
        cols = pl.ds(pl.multiple_of(tile * TD, 128), TD)
        return pltpu.make_async_copy(h_buf.at[slot], h_out.at[:, cols], h_sem.at[slot])

    def fetch_in(tile, slot):
        pltpu.make_async_copy(recv.at[tile], recv.at[tile], recv_sem.at[tile]).wait()
        for copy in in_copies(tile, slot):
            copy.start()

    for copy in (*x_copies(0), *gate_copies(0, 0), *gate_copies(1, 1)):
        copy.start()
    barrier = pltpu.get_barrier_semaphore()
    for peer in (partner, *far):
        pl.semaphore_signal(barrier, inc=1, device_id={"tp": peer}, device_id_type=MESH)
    pl.semaphore_wait(barrier, 3)

    for k in range(n_chunks):
        rows = sum(size for _, _, _, size in chunks[k])
        last = k == n_chunks - 1
        for copy in x_copies(k):
            copy.wait()

        def gate_step(i, _, k=k, rows=rows):
            slot = lax.rem(k * nf + i, 2)
            for copy in gate_copies(i, slot):
                copy.wait()
            for piece in range(TF // 128):
                cols = slice(piece * 128, piece * 128 + 128)
                both = jnp.concatenate([gate_buf[slot, :, cols], up_buf[slot, :, cols]], axis=1)
                prod = jnp.dot(x[0:rows, :], both, preferred_element_type=jnp.float32)
                val = (jax.nn.silu(prod[:, :128]) * prod[:, 128:]).astype(jnp.bfloat16)
                hidden[0:rows, pl.ds(pl.multiple_of(i * TF + piece * 128, 128), 128)] = val
            if k == 0:

                @pl.when(i == nf - 4)
                def _():
                    for tile in (0, 1):
                        down_copy(tile, tile).start()
            else:

                @pl.when(i == 0)
                def _():
                    flush(k - 1, nd - 1, (nd - 1) % 2)

            if k == n_chunks - 1:

                @pl.when(i + 2 < nf)
                def _():
                    for copy in gate_copies(i + 2, slot):
                        copy.start()
            else:
                for copy in gate_copies(lax.rem(i + 2, nf), slot):
                    copy.start()
            return 0

        lax.fori_loop(0, nf, gate_step, 0)
        if not last:
            for copy in x_copies(k + 1):
                copy.start()
        else:
            fetch_in(0, 0)

        if last:
            break

        def down_step(j, _, k=k, rows=rows):
            slot = lax.rem(j, 2)
            down_copy(j, slot).wait()
            y_buf[slot, 0:rows] = jnp.dot(hidden[0:rows, :], down_buf[slot], preferred_element_type=jnp.float32).astype(jnp.bfloat16)

            @pl.when(j > 0)
            def _():
                flush(k, j - 1, 1 - slot)

            for copy in stage_copies(k, j, slot):
                copy.start()
            down_copy(lax.rem(j + 2, nd), slot).start()
            return 0

        lax.fori_loop(0, nd, down_step, 0)

    def own_dot(slot):
        y_buf[slot, 0:block] = jnp.dot(hidden[0:block, :], down_buf[slot], preferred_element_type=jnp.float32).astype(jnp.bfloat16)

    def combine(slot):
        total = y_buf[slot, 0:block].astype(jnp.float32) + in_buf[slot, 2].astype(jnp.float32)
        total = total + in_buf[slot, 0].astype(jnp.float32) + in_buf[slot, 1].astype(jnp.float32)
        h = res_buf[slot].astype(jnp.float32) + total
        h_buf[slot] = h
        sq = h * h
        acc = sq_buf[...]
        for c in range(TD // 128):
            acc = acc + sq[:, c * 128 : c * 128 + 128]
        sq_buf[...] = acc

    sq_buf[...] = jnp.zeros_like(sq_buf)
    down_copy(0, 0).wait()
    own_dot(0)
    down_copy(2, 0).start()
    fetch_in(1, 1)

    def own_step(j, _):
        slot = lax.rem(j, 2)
        down_copy(j, slot).wait()
        for copy in in_copies(j - 1, 1 - slot):
            copy.wait()

        @pl.when(j >= 3)
        def _():
            h_copy(j - 3, 1 - slot).wait()

        combine(1 - slot)
        own_dot(slot)
        h_copy(j - 1, 1 - slot).start()

        @pl.when(j + 2 < nd)
        def _():
            down_copy(j + 2, slot).start()

        @pl.when(j + 2 < nd)
        def _():
            fetch_in(j + 1, 1 - slot)

        return 0

    lax.fori_loop(1, nd, own_step, 0)
    end = (nd - 1) % 2
    fetch_in(nd - 1, end)
    for copy in in_copies(nd - 1, end):
        copy.wait()
    h_copy(nd - 3, end).wait()
    combine(end)
    h_copy(nd - 1, end).start()
    sq_copy = pltpu.make_async_copy(sq_buf, sq_out, sq_sem)
    sq_copy.start()
    h_copy(nd - 2, 1 - end).wait()
    h_copy(nd - 1, end).wait()
    sq_copy.wait()
    pltpu.make_async_copy(stage, stage, send_sem).wait()


def block_sum(x_in, w_gate, w_up, w_down, residual):
    d_model, d_hidden = w_gate.shape
    block = residual.shape[0]
    rows = max(block, 2 * max(HALVES))
    nf, nd = d_hidden // TF, d_model // TD
    any_spec = pl.BlockSpec(memory_space=pl.ANY)
    bf16, f32 = jnp.bfloat16, jnp.float32
    dma = pltpu.SemaphoreType.DMA
    return pl.pallas_call(
        functools.partial(block_kernel, nf, nd, block),
        in_specs=[any_spec] * 5,
        out_specs=[any_spec] * 4,
        out_shape=[
            jax.ShapeDtypeStruct((block, d_model), f32),
            jax.ShapeDtypeStruct((block, 128), f32),
            jax.ShapeDtypeStruct((nd, 3, block, TD), bf16),
            jax.ShapeDtypeStruct((nd, 3, block, TD), bf16),
        ],
        scratch_shapes=[
            pltpu.VMEM((rows, d_model), bf16),
            pltpu.VMEM((2, d_model, TF), bf16),
            pltpu.VMEM((2, d_model, TF), bf16),
            pltpu.VMEM((2, d_hidden, TD), bf16),
            pltpu.VMEM((rows, d_hidden), bf16),
            pltpu.VMEM((2, rows, TD), bf16),
            pltpu.VMEM((2, 3, block, TD), bf16),
            pltpu.VMEM((2, block, TD), bf16),
            pltpu.VMEM((2, block, TD), f32),
            pltpu.VMEM((block, 128), f32),
            dma((2,)),
            dma((2, 2)),
            dma((2, 2)),
            dma((2,)),
            dma((2, 2)),
            dma,
            dma((nd,)),
            dma((2,)),
            dma((2,)),
            dma((2,)),
            dma,
        ],
        compiler_params=pltpu.CompilerParams(vmem_limit_bytes=VMEM, collective_id=0, has_side_effects=True),
        cost_estimate=pl.CostEstimate(flops=24 * block * d_model * d_hidden, bytes_accessed=36 * d_model * d_hidden, transcendentals=0),
        name="block_sum",
    )(x_in, w_gate, w_up, w_down, residual)[:2]


def norm_kernel(h_ref, sq, gain, h_out, n_out):
    d_model = h_ref.shape[1]
    h = h_ref[...]
    scale = lax.rsqrt(jnp.sum(sq[...], axis=1, keepdims=True) / d_model + EPS)
    h_out[...] = h.astype(jnp.bfloat16)
    n_out[...] = (h * scale * gain[...]).astype(jnp.bfloat16)


def norm_rows(h, sq, gain):
    block, d_model = h.shape
    rows = 128
    spec = pl.BlockSpec((rows, d_model), lambda i: (i, 0))
    out = jax.ShapeDtypeStruct(h.shape, jnp.bfloat16)
    return pl.pallas_call(
        norm_kernel,
        grid=(block // rows,),
        in_specs=[spec, pl.BlockSpec((rows, 128), lambda i: (i, 0)), pl.BlockSpec((1, d_model), lambda i: (0, 0))],
        out_specs=[spec, spec],
        out_shape=[out, out],
        cost_estimate=pl.CostEstimate(flops=5 * block * d_model, bytes_accessed=8 * block * d_model, transcendentals=block),
        name="norm_rows",
    )(h, sq, gain)


def solution(mesh):
    def local_block(x_in, w_gate, w_up, w_down, residual, norm_gain):
        h, sq = block_sum(x_in, w_gate, w_up, w_down, residual)
        return tuple(norm_rows(h, sq, norm_gain.reshape(1, -1)))

    row_spec = P(("data", "tp"), None)
    return jax.shard_map(local_block, mesh=mesh, in_specs=(P("data", None), P(None, "tp"), P(None, "tp"), P("tp", None), row_spec, P(None)), out_specs=(row_spec, row_spec), check_vma=False)
```
